256 devices in a mesh: outer: 16 (over x_lo, y, core), inner: 16 (over z, x_hi).
Axes of the slice: x: 4 (x_hi: 2, x_lo: 2; x = x_hi * 2 + x_lo), y: 4, z: 8, core: 2. Of those that a mesh axis runs over, the one named last changes fastest.
Arguments:
- query_image: bfloat16 [8192, 2048], P(('outer', 'inner')), may hold values from -6 to 6
- key_image: bfloat16 [8192, 2048], P(('outer', 'inner')), may hold values from -6 to 6
- value_image: bfloat16 [8192, 2048], P(('outer', 'inner')), may hold values from -6 to 6
- attended_image: bfloat16 [8192, 2048], P(('outer', 'inner')), may hold values from -6 to 6
- upstream_image: bfloat16 [8192, 2048], P(('outer', 'inner')), may hold values from -128 to 128
- logsum_image: float32 [8192, 16], P(('outer', 'inner')), may hold values from 8.6 to 9.4
- query_text: bfloat16 [512, 2048], P(None, 'outer'), may hold values from -6 to 6
- key_text: bfloat16 [512, 2048], P(None, 'outer'), may hold values from -6 to 6
- value_text: bfloat16 [512, 2048], P(None, 'outer'), may hold values from -6 to 6
- attended_text: bfloat16 [512, 2048], P(None, 'outer'), may hold values from -6 to 6
- upstream_text: bfloat16 [512, 2048], P(None, 'outer'), may hold values from -128 to 128
- logsum_text: float32 [512, 16], P(None, 'outer'), may hold values from 8.6 to 9.4
Outputs:
- grad_query_image: bfloat16 [8192, 2048], P(('outer', 'inner'))
- grad_key_image: bfloat16 [8192, 2048], P(('outer', 'inner'))
- grad_value_image: bfloat16 [8192, 2048], P(('outer', 'inner'))
- grad_query_text: bfloat16 [512, 2048], P('inner', 'outer')
- grad_key_text: bfloat16 [512, 2048], P('inner', 'outer')
- grad_value_text: bfloat16 [512, 2048], P('inner', 'outer')
The draws below stay inside these ranges and needn't reach their ends.
All inputs are finite; a program needn't handle non-finite values.
Results may differ from the reference program's by a relative error of at most 0.0055.
Values may be sent and summed in bfloat16 or wider, within the bound.
No kernel may reach another device: no remote copies, remote signals or barrier semaphores. Data moves between devices by JAX's collectives and lax.ppermute only.
A program may use at most 64 MiB of HBM per device.

```python
import jax
import jax.numpy as jnp
from jax import lax

HEAD_DIM = 128
TEXT = 512
TOK_DEV = 512
HEADS = 16
IMAGE = 8192
WIDTH = 2048
N_INNER = 16


def block_scale(stream_key, extent, cuts, low, top_value):
    gain, own = 1.0, jax.random.fold_in(stream_key, 6)
    for dim, blocks in cuts:
        steps = jnp.exp(jax.random.uniform(jax.random.fold_in(own, dim), (blocks,), jnp.float32, low / len(cuts), top_value / len(cuts)))
        gain = gain * jnp.repeat(steps, extent[dim] // blocks).reshape([-1 if axis == dim else 1 for axis in range(len(extent))])
    return gain


def scatter_about(rng, shape, spread, bound, pieces=(), kind=jnp.bfloat16):
    values = jax.random.normal(rng, shape, jnp.float32) * spread
    if len(pieces) > 0:
        values = block_scale(rng, shape, pieces, -0.22, 0.18) * values
    return jnp.clip(values, min=-bound, max=bound).astype(kind)


def setup_inputs(seed: int = 0) -> dict:
    key_of = jax.random.split(jax.random.key(seed), 13)
    return {
        "query_image": scatter_about(key_of[0], (IMAGE, WIDTH), 1.0, 6.0, ((0, 256),)),
        "key_image": scatter_about(key_of[1], (IMAGE, WIDTH), 1.0, 6.0, ((0, 256),)),
        "value_image": scatter_about(key_of[2], (IMAGE, WIDTH), 1.0, 6.0, ((0, 256),)),
        "attended_image": scatter_about(key_of[3], (IMAGE, WIDTH), 1.0, 6.0, ((0, 256),)),
        "upstream_image": scatter_about(key_of[4], (IMAGE, WIDTH), 24.0, 128.0, ((0, 256),)),
        "logsum_image": jnp.clip(8.6 + 0.79999924 * jax.random.uniform(key_of[5], (IMAGE, HEADS), jnp.float32) ** block_scale(key_of[5], (IMAGE, HEADS), ((0, 256),), -0.2, 0.2), 8.6, 9.4),
        "query_text": scatter_about(key_of[6], (TEXT, WIDTH), 1.0, 6.0, ((1, 16),)),
        "key_text": scatter_about(key_of[7], (TEXT, WIDTH), 1.0, 6.0, ((1, 16),)),
        "value_text": scatter_about(key_of[8], (TEXT, WIDTH), 1.0, 6.0, ((1, 16),)),
        "attended_text": scatter_about(key_of[9], (TEXT, WIDTH), 1.0, 6.0, ((1, 16),)),
        "upstream_text": scatter_about(key_of[10], (TEXT, WIDTH), 24.0, 128.0, ((1, 16),)),
        "logsum_text": jnp.clip(8.6 + 0.79999924 * jax.random.uniform(key_of[11], (TEXT, HEADS), jnp.float32) ** block_scale(key_of[11], (TEXT, HEADS), ((1, 16),), -0.2, 0.2), 8.6, 9.4),
    }


def weights_and_mixed(queries, upstream, log_sums, deltas, keys, values):
    scores = jnp.dot(queries, keys.T, preferred_element_type=jnp.float32) * (HEAD_DIM ** -0.5)
    weights = jnp.exp(scores - log_sums)
    slopes = jnp.dot(upstream, values.T, preferred_element_type=jnp.float32)
    mixed = weights * (slopes - deltas)
    return weights.astype(jnp.bfloat16), mixed.astype(jnp.bfloat16)


def query_side(mixed_half, keys):
    return jnp.dot(mixed_half, keys, preferred_element_type=jnp.float32) * (HEAD_DIM ** -0.5)


def key_side(weights_half, mixed_half, queries, upstream):
    grad_values = jnp.dot(weights_half.T, upstream, preferred_element_type=jnp.float32)
    grad_keys = jnp.dot(mixed_half.T, queries, preferred_element_type=jnp.float32) * (HEAD_DIM ** -0.5)
    return grad_keys, grad_values


def reference(query_image, key_image, value_image, attended_image, upstream_image, logsum_image,
              query_text, key_text, value_text, attended_text, upstream_text, logsum_text):
    queries = jnp.concatenate([query_text, query_image], axis=0)
    keys = jnp.concatenate([key_text, key_image], axis=0)
    values = jnp.concatenate([value_text, value_image], axis=0)
    attended = jnp.concatenate([attended_text, attended_image], axis=0)
    upstream = jnp.concatenate([upstream_text, upstream_image], axis=0)
    log_sums = jnp.concatenate([logsum_text, logsum_image], axis=0)
    total = TEXT + IMAGE

    def one_head(head):
        start = head * HEAD_DIM

        def columns(matrix):
            return lax.dynamic_slice_in_dim(matrix, start, HEAD_DIM, 1)

        head_q = columns(queries)
        head_k = columns(keys)
        head_v = columns(values)
        head_g = columns(upstream)
        head_o = columns(attended)
        head_l = lax.dynamic_slice_in_dim(log_sums, head, 1, 1)
        head_delta = jnp.sum(head_g.astype(jnp.float32) * head_o.astype(jnp.float32), axis=1, keepdims=True)
        empty = jnp.zeros((total, HEAD_DIM), jnp.float32)

        def block_back(carry, block):
            block_q, block_g, block_l, block_d = block
            weights_half, mixed_half = weights_and_mixed(block_q, block_g, block_l, block_d, head_k, head_v)
            grad_q = query_side(mixed_half, head_k)
            grad_k, grad_v = key_side(weights_half, mixed_half, block_q, block_g)
            return (carry[0] + grad_k, carry[1] + grad_v), grad_q

        carry, text_q = block_back((empty, empty), (head_q[:TEXT], head_g[:TEXT], head_l[:TEXT], head_delta[:TEXT]))
        blocks = tuple(item[TEXT:].reshape((N_INNER, TOK_DEV) + item.shape[1:])
                       for item in (head_q, head_g, head_l, head_delta))
        (grad_k, grad_v), image_q = lax.scan(block_back, carry, blocks)
        grad_q = jnp.concatenate([text_q, image_q.reshape(IMAGE, HEAD_DIM)], axis=0)
        return grad_q, grad_k, grad_v

    grad_q, grad_k, grad_v = lax.map(one_head, jnp.arange(HEADS, dtype=jnp.int32))

    def join_heads(stacked):
        return jnp.transpose(stacked, (1, 0, 2)).reshape(total, HEADS * HEAD_DIM).astype(jnp.bfloat16)

    grad_q = join_heads(grad_q)
    grad_k = join_heads(grad_k)
    grad_v = join_heads(grad_v)
    return (grad_q[TEXT:], grad_k[TEXT:], grad_v[TEXT:],
            grad_q[:TEXT], grad_k[:TEXT], grad_v[:TEXT])
```

```python
import functools

import jax
import jax.numpy as jnp
from jax import lax
from jax.experimental import pallas as pl
from jax.experimental.pallas import tpu as pltpu
from jax.sharding import PartitionSpec as P


HEAD_DIM = 128
HEADS = 16
RING = 8
TOK = 32
NEAR = 512
OWN = NEAR + TOK
CHUNK = 136
SCALE = HEAD_DIM**-0.5
LOG2E = 1.4426950408889634
F32 = jnp.float32
BF16 = jnp.bfloat16
VM = pl.BlockSpec(memory_space=pltpu.VMEM)
SM = pl.BlockSpec(memory_space=pltpu.SMEM)


def nt(a, b):
    return lax.dot_general(a, b, (((1,), (1,)), ((), ())), preferred_element_type=F32)


def nn(a, b):
    return lax.dot_general(a, b, (((1,), (0,)), ((), ())), preferred_element_type=F32)


def tn(a, b):
    return lax.dot_general(a, b, (((0,), (0,)), ((), ())), preferred_element_type=F32)


def three_pieces(x):
    first = x.astype(BF16)
    rest = x - first.astype(F32)
    second = rest.astype(BF16)
    third = (rest - second.astype(F32)).astype(BF16)
    return first.astype(F32), second.astype(F32), third.astype(F32)


def pack_body(where, q, k, v, o, g, logs, out, rows):
    slot = where[2]
    lane_head = lax.broadcasted_iota(jnp.int32, (TOK, 128), 1)
    sums = jnp.zeros((TOK, 128), F32)
    for h in range(HEADS):
        cols = slice(h * 128, (h + 1) * 128)
        out[h, 0:32, :] = q[:, cols]
        out[h, 32:64, :] = g[:, cols]
        out[h, 64:96, :] = k[:, cols]
        out[h, 96:128, :] = v[:, cols]
        product = g[:, cols].astype(F32) * o[:, cols].astype(F32)
        sums = jnp.where(lane_head == h, jnp.sum(product, axis=1, keepdims=True), sums)
    deltas = jnp.transpose(jnp.concatenate([sums] * 4, axis=0))[0:HEADS]
    logs4 = jnp.concatenate([logs[...] * LOG2E] * 4, axis=1)
    mine = lax.broadcasted_iota(jnp.int32, (HEADS, 128), 1) // TOK == slot
    pieces = three_pieces(jnp.where(mine, logs4, 0.0)) + three_pieces(jnp.where(mine, deltas, 0.0))
    rows[...] = jnp.zeros_like(rows)
    for h in range(HEADS):
        for n, piece in enumerate(pieces):
            rows[h, n : n + 1, :] = piece[h : h + 1, :]
    for h in range(HEADS):
        out[h, 128:136, :] = rows[h].astype(BF16)


def unpack_body(got, qg, kv):
    for o in range(HEADS):
        at = slice(o * TOK, (o + 1) * TOK)
        qg[o * TOK : (o + 1) * TOK, :] = got[o, 0:32, :]
        qg[NEAR + o * TOK : NEAR + (o + 1) * TOK, :] = got[o, 32:64, :]
        kv[o * TOK : (o + 1) * TOK, :] = got[o, 64:96, :]
        kv[NEAR + o * TOK : NEAR + (o + 1) * TOK, :] = got[o, 96:128, :]
    for a in range(4):
        total = got[4 * a, 128:136, :].astype(F32)
        for j in range(1, 4):
            total = total + got[4 * a + j, 128:136, :].astype(F32)
        qg[2 * NEAR + 8 * a : 2 * NEAR + 8 * a + 8, :] = total.astype(BF16)


def one_block(q, g, logs, deltas, chunks, dk, dv):
    total = None
    for keys, values, base, size in chunks:
        k, v = keys(), values()
        weights = jnp.exp2(nt(k, q) * (SCALE * LOG2E) - logs)
        mixed = (weights * (nt(v, g) - deltas)).astype(BF16)
        dv[base : base + size, :] += nn(weights.astype(BF16), g)
        dk[base : base + size, :] += nn(mixed, q)
        part = tn(mixed, k)
        total = part if total is None else total + part
    return total * SCALE


def key_chunks(kv_own, kv_other, text_k, text_v, first_text):
    def piece(ref, start):
        return lambda: ref[start : start + NEAR, :]

    def text(ref):
        return lambda: ref[pl.ds(first_text, 2 * TOK), :]

    return [
        (piece(kv_own, 0), piece(kv_own, NEAR), 0, NEAR),
        (piece(kv_other, 0), piece(kv_other, NEAR), NEAR, NEAR),
        (text(text_k), text(text_v), 2 * NEAR, 2 * TOK),
    ]


def block_operands(qg):
    ld = qg[2 * NEAR : 2 * NEAR + 32, :].astype(F32)
    logs = jnp.concatenate(
        [ld[8 * a : 8 * a + 1] + ld[8 * a + 1 : 8 * a + 2] + ld[8 * a + 2 : 8 * a + 3] for a in range(4)],
        axis=1,
    )
    deltas = jnp.concatenate(
        [ld[8 * a + 3 : 8 * a + 4] + ld[8 * a + 4 : 8 * a + 5] + ld[8 * a + 5 : 8 * a + 6] for a in range(4)],
        axis=1,
    )
    return qg[0:NEAR, :], qg[NEAR : 2 * NEAR, :], logs, deltas


def near_body(where, kv_own, kv_other, text_k, text_v, qg, text_q, text_g, text_ld, dq, dq_text, dk, dv, tq, tg):
    z, side = where[0], where[1]
    chunks = key_chunks(kv_own, kv_other, text_k, text_v, pl.multiple_of(z * 64, 64))
    dk[...] = jnp.zeros_like(dk)
    dv[...] = jnp.zeros_like(dv)
    for n in range(RING):
        rows = pl.ds(pl.multiple_of(n * 64 + side * TOK, TOK), TOK)
        tq[n * TOK : (n + 1) * TOK, :] = text_q[rows, :]
        tg[n * TOK : (n + 1) * TOK, :] = text_g[rows, :]
    dq_text[...] = one_block(
        tq[...], tg[...], text_ld[0:1, :], text_ld[1:2, :], chunks, dk, dv
    ).astype(BF16)
    q, g, logs, deltas = block_operands(qg)
    dq[...] = one_block(q, g, logs, deltas, chunks, dk, dv)


def far_body(count, offsets, last, *refs):
    where, kv_own, kv_other, text_k, text_v, dq_text = refs[:6]
    blocks = refs[6 : 6 + count]
    dk_in, dv_in = refs[6 + count : 8 + count]
    dqs = refs[8 + count : 8 + 2 * count]
    dk, dv = refs[8 + 2 * count : 10 + 2 * count]
    z, side = where[0], where[1]
    chunks = key_chunks(kv_own, kv_other, text_k, text_v, pl.multiple_of(z * 64, 64))
    dk[...] = dk_in[...]
    dv[...] = dv_in[...]
    for qg, dq, offset in zip(blocks, dqs, offsets):
        q, g, logs, deltas = block_operands(qg)
        dq[0:NEAR, :] = one_block(q, g, logs, deltas, chunks, dk, dv).astype(BF16)
        owner = lax.rem(z + offset, RING)
        dq[NEAR:OWN, :] = dq_text[pl.ds(pl.multiple_of(owner * TOK, TOK), TOK), :]
    if last:
        send = refs[10 + 2 * count]
        text = pl.ds(pl.multiple_of(2 * NEAR + (1 - side) * TOK, TOK), TOK)
        for source, lanes, factor in ((dk, slice(0, 128), SCALE), (dv, slice(128, 256), 1.0)):
            send[0:NEAR, lanes] = (source[NEAR : 2 * NEAR, :] * factor).astype(BF16)
            send[NEAR:OWN, lanes] = (source[text, :] * factor).astype(BF16)


def join_body(where, dq, dq_text, dk, dv, kv_got, *refs):
    gots = refs[: RING - 1]
    out, out_q, out_k, out_v = refs[RING - 1 :]
    z, side = where[0], where[1]
    for o in range(HEADS):
        at = slice(o * TOK, (o + 1) * TOK)
        total = dq[at, :]
        for got in gots:
            total = total + got[at, :].astype(F32)
        out[o, 0:32, :] = total.astype(BF16)
        out[o, 32:64, :] = (dk[at, :] * SCALE + kv_got[at, 0:128].astype(F32)).astype(BF16)
        out[o, 64:96, :] = (dv[at, :] + kv_got[at, 128:256].astype(F32)).astype(BF16)
    total = dq_text[pl.ds(pl.multiple_of(z * TOK, TOK), TOK), :].astype(F32)
    for got in gots:
        total = total + got[NEAR:OWN, :].astype(F32)
    out_q[...] = total.astype(BF16)
    text = pl.ds(pl.multiple_of(2 * NEAR + side * TOK, TOK), TOK)
    out_k[...] = (dk[text, :] * SCALE + kv_got[NEAR:OWN, 0:128].astype(F32)).astype(BF16)
    out_v[...] = (dv[text, :] + kv_got[NEAR:OWN, 128:256].astype(F32)).astype(BF16)


def spread_body(got, dq, dk, dv):
    for h in range(HEADS):
        cols = slice(h * 128, (h + 1) * 128)
        dq[:, cols] = got[h, 0:32, :]
        dk[:, cols] = got[h, 32:64, :]
        dv[:, cols] = got[h, 64:96, :]


def kernel(body, name, outs, specs, flops=0, scratch=(), aliases=None):
    return pl.pallas_call(
        body,
        out_shape=outs,
        in_specs=specs,
        out_specs=jax.tree.map(lambda _: VM, outs),
        scratch_shapes=scratch,
        input_output_aliases=aliases or {},
        cost_estimate=pl.CostEstimate(flops=flops, bytes_accessed=1 << 20, transcendentals=0),
        name=name,
    )


def sds(shape, dtype=BF16):
    return jax.ShapeDtypeStruct(shape, dtype)


def block_flops(queries):
    return 10 * queries * 2 * OWN * HEAD_DIM


def shards(
    query_image,
    key_image,
    value_image,
    attended_image,
    upstream_image,
    logsum_image,
    query_text,
    key_text,
    value_text,
    attended_text,
    upstream_text,
    logsum_text,
):
    inner = lax.axis_index("inner").astype(jnp.int32)
    outer = lax.axis_index("outer").astype(jnp.int32)
    z, side = inner // 2, inner % 2
    where = jnp.stack([z, side, outer % 4])

    def along_ring(x, step):
        pairs = [(2 * a + b, 2 * ((a + step) % RING) + b) for a in range(RING) for b in range(2)]
        return lax.ppermute(x, "inner", pairs)

    def across(x):
        return lax.ppermute(x, "inner", [(n, n ^ 1) for n in range(2 * RING)])

    packed = kernel(
        pack_body, "pack", sds((HEADS, CHUNK, 128)), [SM] + [VM] * 6, scratch=[pltpu.VMEM((HEADS, 8, 128), F32)]
    )(where, query_image, key_image, value_image, attended_image, upstream_image, logsum_image.T)
    got = lax.all_to_all(packed, "outer", split_axis=0, concat_axis=0, tiled=True)
    qg, kv = kernel(unpack_body, "unpack", [sds((2 * NEAR + 32, 128)), sds((2 * NEAR, 128))], [VM])(got)

    text_delta = jnp.sum(upstream_text.astype(F32) * attended_text.astype(F32), axis=1)
    text_ld = jnp.stack([logsum_text[:, 0] * LOG2E, text_delta]).reshape(2, RING, 2, TOK)
    text_ld = lax.dynamic_index_in_dim(text_ld, side, 2, keepdims=False).reshape(2, RING * TOK)

    kv_other = across(kv)
    common = (where, kv, kv_other, key_text, value_text)
    acc = sds((2 * OWN, 128), F32)
    dq, dq_text, dk, dv = kernel(
        near_body,
        "near",
        [sds((NEAR, 128), F32), sds((RING * TOK, 128)), acc, acc],
        [SM] + [VM] * 8,
        flops=block_flops(NEAR + RING * TOK),
        scratch=[pltpu.VMEM((RING * TOK, 128), BF16)] * 2,
    )(*common, qg, query_text, upstream_text, text_ld)

    up = down = qg
    returned = []
    for step in range(1, 5):
        up = along_ring(up, 1)
        blocks, offsets = [up], [RING - step]
        if step < 4:
            down = along_ring(down, -1)
            blocks.append(down)
            offsets.append(step)
        count = len(blocks)
        last = step == 4
        outs = [sds((OWN, 128))] * count + [acc, acc] + ([sds((OWN, 256))] if last else [])
        result = kernel(
            functools.partial(far_body, count, offsets, last),
            f"far{step}",
            outs,
            [SM] + [VM] * (7 + count),
            flops=block_flops(NEAR * count),
            aliases={6 + count: count, 7 + count: count + 1},
        )(*common, dq_text, *blocks, dk, dv)
        dk, dv = result[count], result[count + 1]
        for part, offset in zip(result[:count], offsets):
            returned.append(along_ring(part, offset))
        if last:
            kv_got = across(result[count + 2])

    joined, text_dq, text_dk, text_dv = kernel(
        join_body,
        "join",
        [sds((HEADS, 96, 128)), sds((TOK, 128)), sds((TOK, 128)), sds((TOK, 128))],
        [SM] + [VM] * (4 + RING),
    )(where, dq, dq_text, dk, dv, kv_got, *returned)
    home = lax.all_to_all(joined, "outer", split_axis=0, concat_axis=0, tiled=True)
    image = kernel(spread_body, "spread", [sds((TOK, HEADS * 128))] * 3, [VM])(home)
    return (*image, text_dq, text_dk, text_dv)


def solution(mesh):
    image = P(("outer", "inner"), None)
    text = P(None, "outer")
    share = P("inner", "outer")
    return jax.shard_map(
        shards,
        mesh=mesh,
        in_specs=(image,) * 6 + (text,) * 6,
        out_specs=(image,) * 3 + (share,) * 3,
        check_vma=False,
    )
```

```python
import functools

import jax
import jax.numpy as jnp
from jax import lax
from jax.experimental import pallas as pl
from jax.experimental.pallas import tpu as pltpu
from jax.sharding import PartitionSpec as P


HEAD_DIM = 128
HEADS = 16
RING = 8
TOK = 32
NEAR = 512
OWN = NEAR + TOK
CHUNK = 136
SCALE = HEAD_DIM**-0.5
LOG2E = 1.4426950408889634
F32 = jnp.float32
BF16 = jnp.bfloat16
VMEM_LIMIT = 24 << 20
WHOLE_VMEM = 62 << 20
VM = pl.BlockSpec(memory_space=pltpu.VMEM)
HB = pl.BlockSpec(memory_space=pltpu.HBM)


def nt(a, b):
    return lax.dot_general(a, b, (((1,), (1,)), ((), ())), preferred_element_type=F32)


def nn(a, b):
    return lax.dot_general(a, b, (((1,), (0,)), ((), ())), preferred_element_type=F32)


def tn(a, b):
    return lax.dot_general(a, b, (((0,), (0,)), ((), ())), preferred_element_type=F32)


def three_pieces(x):
    first = x.astype(BF16)
    rest = x - first.astype(F32)
    second = rest.astype(BF16)
    third = (rest - second.astype(F32)).astype(BF16)
    return first.astype(F32), second.astype(F32), third.astype(F32)


def place():
    inner = lax.axis_index("inner")
    return inner // 2, lax.rem(inner, 2)


def pack_body(q_in, k_in, v_in, o_in, g_in, logs, out, rows, q, k, v, o, g, sems):
    copies = [
        pltpu.make_async_copy(source, target, sems.at[n])
        for n, (source, target) in enumerate(((g_in, g), (o_in, o), (q_in, q), (k_in, k), (v_in, v)))
    ]
    for copy in copies:
        copy.start()
    for copy in copies:
        copy.wait()
    slot = lax.rem(lax.axis_index("outer"), 4)
    lane_head = lax.broadcasted_iota(jnp.int32, (TOK, 128), 1)
    sums = jnp.zeros((TOK, 128), F32)
    for h in range(HEADS):
        cols = slice(h * 128, (h + 1) * 128)
        out[h, 0:32, :] = q[:, cols]
        out[h, 32:64, :] = g[:, cols]
        out[h, 64:96, :] = k[:, cols]
        out[h, 96:128, :] = v[:, cols]
        product = g[:, cols].astype(F32) * o[:, cols].astype(F32)
        sums = jnp.where(lane_head == h, jnp.sum(product, axis=1, keepdims=True), sums)
    deltas = jnp.transpose(jnp.concatenate([sums] * 4, axis=0))[0:HEADS]
    logs4 = jnp.concatenate([logs[...] * LOG2E] * 4, axis=1)
    mine = lax.broadcasted_iota(jnp.int32, (HEADS, 128), 1) // TOK == slot
    pieces = three_pieces(jnp.where(mine, logs4, 0.0)) + three_pieces(jnp.where(mine, deltas, 0.0))
    rows[...] = jnp.zeros_like(rows)
    for h in range(HEADS):
        for n, piece in enumerate(pieces):
            rows[h, n : n + 1, :] = piece[h : h + 1, :]
    for h in range(HEADS):
        out[h, 128:136, :] = rows[h].astype(BF16)


def unpack_body(got, qg, kv):
    for o in range(HEADS):
        qg[o * TOK : (o + 1) * TOK, :] = got[o, 0:32, :]
        qg[NEAR + o * TOK : NEAR + (o + 1) * TOK, :] = got[o, 32:64, :]
        kv[o * TOK : (o + 1) * TOK, :] = got[o, 64:96, :]
        kv[NEAR + o * TOK : NEAR + (o + 1) * TOK, :] = got[o, 96:128, :]
    for a in range(4):
        total = got[4 * a, 128:136, :].astype(F32)
        for j in range(1, 4):
            total = total + got[4 * a + j, 128:136, :].astype(F32)
        qg[2 * NEAR + 8 * a : 2 * NEAR + 8 * a + 8, :] = total.astype(BF16)


def one_block(q, g, logs, deltas, keys, values, dk, dv):
    total = None
    for base, size in ((0, NEAR), (NEAR, 2 * OWN - NEAR)):
        k, v = keys[base : base + size, :], values[base : base + size, :]
        weights = jnp.exp2(nt(k, q) * (SCALE * LOG2E) - logs)
        mixed = (weights * (nt(v, g) - deltas)).astype(BF16)
        dv[base : base + size, :] += nn(weights.astype(BF16), g)
        dk[base : base + size, :] += nn(mixed, q)
        part = tn(mixed, k)
        total = part if total is None else total + part
    return total * SCALE


def block_operands(qg):
    ld = qg[2 * NEAR : 2 * NEAR + 32, :].astype(F32)
    logs = jnp.concatenate(
        [ld[8 * a : 8 * a + 1] + ld[8 * a + 1 : 8 * a + 2] + ld[8 * a + 2 : 8 * a + 3] for a in range(4)],
        axis=1,
    )
    deltas = jnp.concatenate(
        [ld[8 * a + 3 : 8 * a + 4] + ld[8 * a + 4 : 8 * a + 5] + ld[8 * a + 5 : 8 * a + 6] for a in range(4)],
        axis=1,
    )
    return qg[0:NEAR, :], qg[NEAR : 2 * NEAR, :], logs, deltas


def text_body(kv_own, kv_other, text_k, text_v, text_q, text_g, text_ld, dq_text, dk, dv, keys, values, tq, tg):
    z, side = place()
    for target, start, text in ((keys, 0, text_k), (values, NEAR, text_v)):
        target[0:NEAR, :] = kv_own[start : start + NEAR, :]
        target[NEAR : 2 * NEAR, :] = kv_other[start : start + NEAR, :]
        target[2 * NEAR : 2 * OWN, :] = text[pl.ds(pl.multiple_of(z * 64, 64), 2 * TOK), :]
    dk[...] = jnp.zeros_like(dk)
    dv[...] = jnp.zeros_like(dv)
    for n in range(RING):
        rows = pl.ds(pl.multiple_of(n * 64 + side * TOK, TOK), TOK)
        tq[n * TOK : (n + 1) * TOK, :] = text_q[rows, :]
        tg[n * TOK : (n + 1) * TOK, :] = text_g[rows, :]
    logs, deltas = text_ld[pl.ds(side, 1), :], text_ld[pl.ds(2 + side, 1), :]
    dq_text[...] = one_block(tq[...], tg[...], logs, deltas, keys, values, dk, dv).astype(BF16)


def own_body(keys, values, qg, dk_in, dv_in, dq, dk, dv):
    dk[...] = dk_in[...]
    dv[...] = dv_in[...]
    q, g, logs, deltas = block_operands(qg)
    dq[...] = one_block(q, g, logs, deltas, keys, values, dk, dv)


def far_body(step, *refs):
    keys, values, dq_text = refs[:3]
    z, side = place()
    count = 2 if step < 4 else 1
    blocks, refs = refs[3 : 3 + count], refs[3 + count :]
    (dk_in, dv_in), refs = refs[:2], refs[2:]
    if step == 3:
        firsts, refs = refs[:2], refs[2:]
    dqs, refs = refs[:count], refs[count:]
    (dk, dv), refs = refs[:2], refs[2:]
    dk[...] = dk_in[...]
    dv[...] = dv_in[...]
    for n, (qg, dq) in enumerate(zip(blocks, dqs)):
        q, g, logs, deltas = block_operands(qg)
        dq[0:NEAR, :] = one_block(q, g, logs, deltas, keys, values, dk, dv).astype(dq.dtype)
        owner = lax.rem(z + (step if n == 1 else RING - step), RING)
        text = dq_text[pl.ds(pl.multiple_of(owner * TOK, TOK), TOK), :]
        dq[NEAR:OWN, :] = text.astype(dq.dtype)
        if step == 3:
            dq[OWN : 2 * OWN, :] = firsts[n][...]
    if step == 4:
        (send,) = refs
        text = pl.ds(pl.multiple_of(2 * NEAR + (1 - side) * TOK, TOK), TOK)
        for source, lanes, factor in ((dk, slice(0, 128), SCALE), (dv, slice(128, 256), 1.0)):
            send[0:NEAR, lanes] = (source[NEAR : 2 * NEAR, :] * factor).astype(BF16)
            send[NEAR:OWN, lanes] = (source[text, :] * factor).astype(BF16)


def mid_body(mine, *refs):
    total = mine[...]
    for got in refs[:-1]:
        total = total + got[0:OWN, :].astype(F32)
    refs[-1][...] = total.astype(BF16)


def join_body(dq, dq_text, dk, dv, kv_got, from_low, from_high, *refs):
    gots = refs[:2]
    out, out_q, out_k, out_v = refs[2:]
    z, side = place()

    def arrived(total, start, size):
        for got, base in ((from_low, OWN), (from_high, OWN), *((got, 0) for got in gots)):
            total = total + got[base + start : base + start + size, :].astype(F32)
        return total.astype(BF16)

    for o in range(HEADS):
        at = slice(o * TOK, (o + 1) * TOK)
        out[o, 0:32, :] = arrived(dq[at, :], o * TOK, TOK)
        out[o, 32:64, :] = (dk[at, :] * SCALE + kv_got[at, 0:128].astype(F32)).astype(BF16)
        out[o, 64:96, :] = (dv[at, :] + kv_got[at, 128:256].astype(F32)).astype(BF16)
    own_text = dq_text[pl.ds(pl.multiple_of(z * TOK, TOK), TOK), :].astype(F32)
    out_q[...] = arrived(own_text, NEAR, TOK)
    text = pl.ds(pl.multiple_of(2 * NEAR + side * TOK, TOK), TOK)
    out_k[...] = (dk[text, :] * SCALE + kv_got[NEAR:OWN, 0:128].astype(F32)).astype(BF16)
    out_v[...] = (dv[text, :] + kv_got[NEAR:OWN, 128:256].astype(F32)).astype(BF16)


def spread_body(got, dq, dk, dv):
    for h in range(HEADS):
        cols = slice(h * 128, (h + 1) * 128)
        dq[:, cols] = got[h, 0:32, :]
        dk[:, cols] = got[h, 32:64, :]
        dv[:, cols] = got[h, 64:96, :]


def kernel(body, outs, count, flops=0, scratch=(), aliases=None, limit=VMEM_LIMIT):
    return pl.pallas_call(
        body,
        out_shape=outs,
        in_specs=count if isinstance(count, list) else [VM] * count,
        out_specs=jax.tree.map(lambda _: VM, outs),
        scratch_shapes=scratch,
        input_output_aliases=aliases or {},
        cost_estimate=pl.CostEstimate(flops=flops, bytes_accessed=1 << 20, transcendentals=0),
        compiler_params=pltpu.CompilerParams(vmem_limit_bytes=limit),
    )


def sds(shape, dtype=BF16):
    return jax.ShapeDtypeStruct(shape, dtype)


def block_flops(queries):
    return 10 * queries * 2 * OWN * HEAD_DIM


def shards(
    query_image,
    key_image,
    value_image,
    attended_image,
    upstream_image,
    logsum_image,
    query_text,
    key_text,
    value_text,
    attended_text,
    upstream_text,
    logsum_text,
):
    def along_ring(x, step):
        pairs = [(2 * z + side, 2 * ((z + step) % RING) + side) for z in range(RING) for side in range(2)]
        return lax.ppermute(x, "inner", pairs)

    def exchanged(x):
        return lax.all_to_all(x, "outer", split_axis=0, concat_axis=0, tiled=True)

    def across(x):
        return lax.ppermute(x, "inner", [(n, n ^ 1) for n in range(2 * RING)])

    packed = kernel(
        pack_body,
        sds((HEADS, CHUNK, 128)),
        [HB] * 5 + [VM],
        scratch=[pltpu.VMEM((HEADS, 8, 128), F32)]
        + [pltpu.VMEM((TOK, HEADS * 128), BF16)] * 5
        + [pltpu.SemaphoreType.DMA((5,))],
        limit=WHOLE_VMEM,
    )(query_image, key_image, value_image, attended_image, upstream_image, logsum_image.T)
    got = exchanged(packed)
    qg, kv = kernel(unpack_body, [sds((2 * NEAR + 32, 128)), sds((2 * NEAR, 128))], 1)(got)

    text_delta = jnp.sum(upstream_text.astype(F32) * attended_text.astype(F32), axis=1)
    text_ld = jnp.stack([logsum_text[:, 0] * LOG2E, text_delta]).reshape(2, RING, 2, TOK)
    text_ld = text_ld.transpose(0, 2, 1, 3).reshape(4, RING * TOK)

    kv_other = across(kv)
    acc = sds((2 * OWN, 128), F32)
    dq_text, dk, dv, keys, values = kernel(
        text_body,
        [sds((RING * TOK, 128)), acc, acc, sds((2 * OWN, 128)), sds((2 * OWN, 128))],
        7,
        flops=block_flops(RING * TOK),
        scratch=[pltpu.VMEM((RING * TOK, 128), BF16)] * 2,
    )(kv, kv_other, key_text, value_text, query_text, upstream_text, text_ld)

    up = down = qg
    parts = {}
    for step in range(1, 5):
        up = along_ring(up, 1)
        blocks = [up]
        if step < 4:
            down = along_ring(down, -1)
            blocks.append(down)
        count = len(blocks)
        part = {1: sds((OWN, 128)), 2: sds((OWN, 128), F32), 3: sds((2 * OWN, 128)), 4: sds((OWN, 128))}[step]
        result = kernel(
            functools.partial(far_body, step),
            [part] * count + [acc, acc] + ([sds((OWN, 256))] if step == 4 else []),
            5 + count + (2 if step == 3 else 0),
            flops=block_flops(NEAR * count),
            aliases={3 + count: count, 4 + count: count + 1},
        )(keys, values, dq_text, *blocks, dk, dv, *(parts[1] if step == 3 else ()))
        parts[step] = result[:count]
        dk, dv = result[count : count + 2]
        if step == 2:
            dq, dk, dv = kernel(
                own_body, [sds((NEAR, 128), F32), acc, acc], 5, flops=block_flops(NEAR), aliases={3: 1, 4: 2}
            )(keys, values, qg, dk, dv)
    kv_got = across(result[-1])
    from_high = along_ring(parts[3][0], -1)
    from_low = along_ring(parts[3][1], 1)
    from_far = along_ring(parts[4][0], -2)
    low, high = parts[2]
    high = kernel(mid_body, sds((OWN, 128)), 2)(high, from_low)
    back2 = along_ring(high, 2)
    low = kernel(mid_body, sds((OWN, 128)), 3)(low, from_high, from_far)
    back6 = along_ring(low, -2)

    joined, text_dq, text_dk, text_dv = kernel(
        join_body, [sds((HEADS, 96, 128)), sds((TOK, 128)), sds((TOK, 128)), sds((TOK, 128))], 9
    )(dq, dq_text, dk, dv, kv_got, from_low, from_high, back6, back2)
    home = exchanged(joined)
    image = kernel(spread_body, [sds((TOK, HEADS * 128))] * 3, 1)(home)
    return (*image, text_dq, text_dk, text_dv)


def solution(mesh):
    image = P(("outer", "inner"), None)
    text = P(None, "outer")
    share = P("inner", "outer")

    return jax.shard_map(
        shards,
        mesh=mesh,
        in_specs=(image,) * 6 + (text,) * 6,
        out_specs=(image,) * 3 + (share,) * 3,
        check_vma=False,
    )
```

```python
import functools

import jax
import jax.numpy as jnp
from jax import lax
from jax.experimental import pallas as pl
from jax.experimental.pallas import tpu as pltpu
from jax.sharding import PartitionSpec as P


HEAD_DIM = 128
HEADS = 16
RING = 8
TOK = 32
NEAR = 512
OWN = NEAR + TOK
CHUNK = 136
SCALE = HEAD_DIM**-0.5
LOG2E = 1.4426950408889634
F32 = jnp.float32
BF16 = jnp.bfloat16
VMEM_LIMIT = 24 << 20
WHOLE_VMEM = 62 << 20
VM = pl.BlockSpec(memory_space=pltpu.VMEM)
HB = pl.BlockSpec(memory_space=pltpu.HBM)


def nt(a, b):
    return lax.dot_general(a, b, (((1,), (1,)), ((), ())), preferred_element_type=F32)


def nn(a, b):
    return lax.dot_general(a, b, (((1,), (0,)), ((), ())), preferred_element_type=F32)


def tn(a, b):
    return lax.dot_general(a, b, (((0,), (0,)), ((), ())), preferred_element_type=F32)


def three_pieces(x):
    first = x.astype(BF16)
    rest = x - first.astype(F32)
    second = rest.astype(BF16)
    third = (rest - second.astype(F32)).astype(BF16)
    return first.astype(F32), second.astype(F32), third.astype(F32)


def place():
    inner = lax.axis_index("inner")
    return inner // 2, lax.rem(inner, 2)


def pack_body(q_in, k_in, v_in, o_in, g_in, logs, out, rows, q, k, v, o, g, sems):
    copies = [
        pltpu.make_async_copy(source, target, sems.at[n])
        for n, (source, target) in enumerate(((g_in, g), (o_in, o), (q_in, q), (k_in, k), (v_in, v)))
    ]
    for copy in copies:
        copy.start()
    for copy in copies:
        copy.wait()
    slot = lax.rem(lax.axis_index("outer"), 4)
    lane_head = lax.broadcasted_iota(jnp.int32, (TOK, 128), 1)
    sums = jnp.zeros((TOK, 128), F32)
    for h in range(HEADS):
        cols = slice(h * 128, (h + 1) * 128)
        out[h, 0:32, :] = q[:, cols]
        out[h, 32:64, :] = g[:, cols]
        out[h, 64:96, :] = k[:, cols]
        out[h, 96:128, :] = v[:, cols]
        product = g[:, cols].astype(F32) * o[:, cols].astype(F32)
        sums = jnp.where(lane_head == h, jnp.sum(product, axis=1, keepdims=True), sums)
    deltas = jnp.transpose(jnp.concatenate([sums] * 4, axis=0))[0:HEADS]
    logs4 = jnp.concatenate([logs[...] * LOG2E] * 4, axis=1)
    mine = lax.broadcasted_iota(jnp.int32, (HEADS, 128), 1) // TOK == slot
    pieces = three_pieces(jnp.where(mine, logs4, 0.0)) + three_pieces(jnp.where(mine, deltas, 0.0))
    rows[...] = jnp.zeros_like(rows)
    for h in range(HEADS):
        for n, piece in enumerate(pieces):
            rows[h, n : n + 1, :] = piece[h : h + 1, :]
    for h in range(HEADS):
        out[h, 128:136, :] = rows[h].astype(BF16)


def unpack_body(got, qg, kv):
    for o in range(HEADS):
        qg[o * TOK : (o + 1) * TOK, :] = got[o, 0:32, :]
        qg[NEAR + o * TOK : NEAR + (o + 1) * TOK, :] = got[o, 32:64, :]
        kv[o * TOK : (o + 1) * TOK, :] = got[o, 64:96, :]
        kv[NEAR + o * TOK : NEAR + (o + 1) * TOK, :] = got[o, 96:128, :]
    for a in range(4):
        total = got[4 * a, 128:136, :].astype(F32)
        for j in range(1, 4):
            total = total + got[4 * a + j, 128:136, :].astype(F32)
        qg[2 * NEAR + 8 * a : 2 * NEAR + 8 * a + 8, :] = total.astype(BF16)


def one_block(q, g, logs, deltas, keys, values, dk, dv):
    total = None
    for base, size in ((0, NEAR), (NEAR, 2 * OWN - NEAR)):
        k, v = keys[base : base + size, :], values[base : base + size, :]
        weights = jnp.exp2(nt(k, q) * (SCALE * LOG2E) - logs)
        mixed = (weights * (nt(v, g) - deltas)).astype(BF16)
        dv[base : base + size, :] += nn(weights.astype(BF16), g)
        dk[base : base + size, :] += nn(mixed, q)
        part = tn(mixed, k)
        total = part if total is None else total + part
    return total * SCALE


def block_operands(qg):
    ld = qg[2 * NEAR : 2 * NEAR + 32, :].astype(F32)
    logs = jnp.concatenate(
        [ld[8 * a : 8 * a + 1] + ld[8 * a + 1 : 8 * a + 2] + ld[8 * a + 2 : 8 * a + 3] for a in range(4)],
        axis=1,
    )
    deltas = jnp.concatenate(
        [ld[8 * a + 3 : 8 * a + 4] + ld[8 * a + 4 : 8 * a + 5] + ld[8 * a + 5 : 8 * a + 6] for a in range(4)],
        axis=1,
    )
    return qg[0:NEAR, :], qg[NEAR : 2 * NEAR, :], logs, deltas


def text_body(kv_own, kv_other, text_k, text_v, text_q, text_g, text_ld, dq_text, dk, dv, keys, values, tq, tg):
    z, side = place()
    for target, start, text in ((keys, 0, text_k), (values, NEAR, text_v)):
        target[0:NEAR, :] = kv_own[start : start + NEAR, :]
        target[NEAR : 2 * NEAR, :] = kv_other[start : start + NEAR, :]
        target[2 * NEAR : 2 * OWN, :] = text[pl.ds(pl.multiple_of(z * 64, 64), 2 * TOK), :]
    dk[...] = jnp.zeros_like(dk)
    dv[...] = jnp.zeros_like(dv)
    for n in range(RING):
        rows = pl.ds(pl.multiple_of(n * 64 + side * TOK, TOK), TOK)
        tq[n * TOK : (n + 1) * TOK, :] = text_q[rows, :]
        tg[n * TOK : (n + 1) * TOK, :] = text_g[rows, :]
    logs, deltas = text_ld[pl.ds(side, 1), :], text_ld[pl.ds(2 + side, 1), :]
    dq_text[...] = one_block(tq[...], tg[...], logs, deltas, keys, values, dk, dv).astype(BF16)


def own_body(keys, values, qg, dk_in, dv_in, dq, dk, dv, send):
    _, side = place()
    dk[...] = dk_in[...]
    dv[...] = dv_in[...]
    q, g, logs, deltas = block_operands(qg)
    dq[...] = one_block(q, g, logs, deltas, keys, values, dk, dv)
    text = pl.ds(pl.multiple_of(2 * NEAR + (1 - side) * TOK, TOK), TOK)
    for source, lanes, factor in ((dk, slice(0, 128), SCALE), (dv, slice(128, 256), 1.0)):
        send[0:NEAR, lanes] = (source[NEAR : 2 * NEAR, :] * factor).astype(BF16)
        send[NEAR:OWN, lanes] = (source[text, :] * factor).astype(BF16)


def far_body(step, offset, *refs):
    keys, values, dq_text, qg, dk_in, dv_in = refs[:6]
    first, refs = (refs[6], refs[7:]) if step == 3 else (None, refs[6:])
    dq, dk, dv = refs[:3]
    z, _ = place()
    dk[...] = dk_in[...]
    dv[...] = dv_in[...]
    q, g, logs, deltas = block_operands(qg)
    dq[0:NEAR, :] = one_block(q, g, logs, deltas, keys, values, dk, dv).astype(dq.dtype)
    owner = lax.rem(z + offset, RING)
    text = dq_text[pl.ds(pl.multiple_of(owner * TOK, TOK), TOK), :]
    dq[NEAR:OWN, :] = text.astype(dq.dtype)
    if step == 3:
        dq[OWN : 2 * OWN, :] = first[...]


def mid_body(mine, *refs):
    total = mine[...]
    for got in refs[:-1]:
        total = total + got[0:OWN, :].astype(F32)
    refs[-1][...] = total.astype(BF16)


def join_body(dq, dq_text, dk, dv, kv_got, from_low, from_high, *refs):
    gots = refs[:2]
    out, out_q, out_k, out_v = refs[2:]
    z, side = place()

    def arrived(total, start, size):
        for got, base in ((from_low, OWN), (from_high, OWN), *((got, 0) for got in gots)):
            total = total + got[base + start : base + start + size, :].astype(F32)
        return total.astype(BF16)

    for o in range(HEADS):
        at = slice(o * TOK, (o + 1) * TOK)
        out[o, 0:32, :] = arrived(dq[at, :], o * TOK, TOK)
        out[o, 32:64, :] = (dk[at, :] * SCALE + kv_got[at, 0:128].astype(F32)).astype(BF16)
        out[o, 64:96, :] = (dv[at, :] + kv_got[at, 128:256].astype(F32)).astype(BF16)
    own_text = dq_text[pl.ds(pl.multiple_of(z * TOK, TOK), TOK), :].astype(F32)
    out_q[...] = arrived(own_text, NEAR, TOK)
    text = pl.ds(pl.multiple_of(2 * NEAR + side * TOK, TOK), TOK)
    out_k[...] = (dk[text, :] * SCALE + kv_got[NEAR:OWN, 0:128].astype(F32)).astype(BF16)
    out_v[...] = (dv[text, :] + kv_got[NEAR:OWN, 128:256].astype(F32)).astype(BF16)


def spread_body(got, dq, dk, dv):
    for h in range(HEADS):
        cols = slice(h * 128, (h + 1) * 128)
        dq[:, cols] = got[h, 0:32, :]
        dk[:, cols] = got[h, 32:64, :]
        dv[:, cols] = got[h, 64:96, :]


def kernel(body, outs, count, flops=0, scratch=(), aliases=None, limit=VMEM_LIMIT):
    return pl.pallas_call(
        body,
        out_shape=outs,
        in_specs=count if isinstance(count, list) else [VM] * count,
        out_specs=jax.tree.map(lambda _: VM, outs),
        scratch_shapes=scratch,
        input_output_aliases=aliases or {},
        cost_estimate=pl.CostEstimate(flops=flops, bytes_accessed=1 << 20, transcendentals=0),
        compiler_params=pltpu.CompilerParams(vmem_limit_bytes=limit),
    )


def sds(shape, dtype=BF16):
    return jax.ShapeDtypeStruct(shape, dtype)


def block_flops(queries):
    return 10 * queries * 2 * OWN * HEAD_DIM


def shards(
    query_image,
    key_image,
    value_image,
    attended_image,
    upstream_image,
    logsum_image,
    query_text,
    key_text,
    value_text,
    attended_text,
    upstream_text,
    logsum_text,
):
    def along_ring(x, step):
        pairs = [(2 * z + side, 2 * ((z + step) % RING) + side) for z in range(RING) for side in range(2)]
        return lax.ppermute(x, "inner", pairs)

    def exchanged(x):
        return lax.all_to_all(x, "outer", split_axis=0, concat_axis=0, tiled=True)

    def across(x):
        return lax.ppermute(x, "inner", [(n, n ^ 1) for n in range(2 * RING)])

    packed = kernel(
        pack_body,
        sds((HEADS, CHUNK, 128)),
        [HB] * 5 + [VM],
        scratch=[pltpu.VMEM((HEADS, 8, 128), F32)]
        + [pltpu.VMEM((TOK, HEADS * 128), BF16)] * 5
        + [pltpu.SemaphoreType.DMA((5,))],
        limit=WHOLE_VMEM,
    )(query_image, key_image, value_image, attended_image, upstream_image, logsum_image.T)
    got = exchanged(packed)
    qg, kv = kernel(unpack_body, [sds((2 * NEAR + 32, 128)), sds((2 * NEAR, 128))], 1)(got)

    text_delta = jnp.sum(upstream_text.astype(F32) * attended_text.astype(F32), axis=1)
    text_ld = jnp.stack([logsum_text[:, 0] * LOG2E, text_delta]).reshape(2, RING, 2, TOK)
    text_ld = text_ld.transpose(0, 2, 1, 3).reshape(4, RING * TOK)

    kv_other = across(kv)
    acc = sds((2 * OWN, 128), F32)
    dq_text, dk, dv, keys, values = kernel(
        text_body,
        [sds((RING * TOK, 128)), acc, acc, sds((2 * OWN, 128)), sds((2 * OWN, 128))],
        7,
        flops=block_flops(RING * TOK),
        scratch=[pltpu.VMEM((RING * TOK, 128), BF16)] * 2,
    )(kv, kv_other, key_text, value_text, query_text, upstream_text, text_ld)

    up = down = qg
    parts = {}
    for step in range(1, 5):
        part = {1: sds((OWN, 128)), 2: sds((OWN, 128), F32), 3: sds((2 * OWN, 128)), 4: sds((OWN, 128))}[step]
        parts[step] = []
        up = along_ring(up, 1)
        if step < 4:
            down = along_ring(down, -1)
        for n, moved in enumerate((up, down) if step < 4 else (up,)):
            result = kernel(
                functools.partial(far_body, step, step if n else RING - step),
                [part, acc, acc],
                7 if step == 3 else 6,
                flops=block_flops(NEAR),
                aliases={4: 1, 5: 2},
            )(keys, values, dq_text, moved, dk, dv, *(parts[1][n : n + 1] if step == 3 else ()))
            parts[step].append(result[0])
            dk, dv = result[1:3]
    dq, dk, dv, send = kernel(
        own_body, [sds((NEAR, 128), F32), acc, acc, sds((OWN, 256))], 5, flops=block_flops(NEAR), aliases={3: 1, 4: 2}
    )(keys, values, qg, dk, dv)
    kv_got = across(send)
    from_high = along_ring(parts[3][0], -1)
    from_low = along_ring(parts[3][1], 1)
    from_far = along_ring(parts[4][0], -2)
    low, high = parts[2]
    high = kernel(mid_body, sds((OWN, 128)), 2)(high, from_low)
    back2 = along_ring(high, 2)
    low = kernel(mid_body, sds((OWN, 128)), 3)(low, from_high, from_far)
    back6 = along_ring(low, -2)

    joined, text_dq, text_dk, text_dv = kernel(
        join_body, [sds((HEADS, 96, 128)), sds((TOK, 128)), sds((TOK, 128)), sds((TOK, 128))], 9
    )(dq, dq_text, dk, dv, kv_got, from_low, from_high, back6, back2)
    home = exchanged(joined)
    image = kernel(spread_body, [sds((TOK, HEADS * 128))] * 3, 1)(home)
    return (*image, text_dq, text_dk, text_dv)


def solution(mesh):
    image = P(("outer", "inner"), None)
    text = P(None, "outer")
    share = P("inner", "outer")

    return jax.shard_map(
        shards,
        mesh=mesh,
        in_specs=(image,) * 6 + (text,) * 6,
        out_specs=(image,) * 3 + (share,) * 3,
        check_vma=False,
    )
```

```python
import functools

import jax
import jax.numpy as jnp
from jax import lax
from jax.experimental import pallas as pl
from jax.experimental.pallas import tpu as pltpu
from jax.sharding import PartitionSpec as P


HEAD_DIM = 128
HEADS = 16
RING = 8
TOK = 32
NEAR = 512
OWN = NEAR + TOK
CHUNK = 136
SCALE = HEAD_DIM**-0.5
LOG2E = 1.4426950408889634
F32 = jnp.float32
BF16 = jnp.bfloat16
VMEM_LIMIT = 24 << 20
WHOLE_VMEM = 62 << 20
VM = pl.BlockSpec(memory_space=pltpu.VMEM)
HB = pl.BlockSpec(memory_space=pltpu.HBM)


def nt(a, b):
    return lax.dot_general(a, b, (((1,), (1,)), ((), ())), preferred_element_type=F32)


def nn(a, b):
    return lax.dot_general(a, b, (((1,), (0,)), ((), ())), preferred_element_type=F32)


def tn(a, b):
    return lax.dot_general(a, b, (((0,), (0,)), ((), ())), preferred_element_type=F32)


def three_pieces(x):
    first = x.astype(BF16)
    rest = x - first.astype(F32)
    second = rest.astype(BF16)
    third = (rest - second.astype(F32)).astype(BF16)
    return first.astype(F32), second.astype(F32), third.astype(F32)


def place():
    inner = lax.axis_index("inner")
    return inner // 2, lax.rem(inner, 2)


def pack_body(q_in, k_in, v_in, o_in, g_in, logs_in, out, rows, q, k, v, o, g, logs, sems):
    copies = [
        pltpu.make_async_copy(source, target, sems.at[n])
        for n, (source, target) in enumerate(
            ((g_in, g), (o_in, o), (logs_in, logs), (q_in, q), (k_in, k), (v_in, v))
        )
    ]
    for copy in copies:
        copy.start()
    for copy in copies:
        copy.wait()
    slot = lax.rem(lax.axis_index("outer"), 4)
    lane_head = lax.broadcasted_iota(jnp.int32, (TOK, 128), 1)
    sums = jnp.zeros((TOK, 128), F32)
    for h in range(HEADS):
        cols = slice(h * 128, (h + 1) * 128)
        out[h, 0:32, :] = q[:, cols]
        out[h, 32:64, :] = g[:, cols]
        out[h, 64:96, :] = k[:, cols]
        out[h, 96:128, :] = v[:, cols]
        product = g[:, cols].astype(F32) * o[:, cols].astype(F32)
        sums = jnp.where(lane_head == h, jnp.sum(product, axis=1, keepdims=True), sums)
    deltas = jnp.transpose(jnp.concatenate([sums] * 4, axis=0))[0:HEADS]
    logs4 = jnp.concatenate([logs[...] * LOG2E] * 4, axis=1)
    mine = lax.broadcasted_iota(jnp.int32, (HEADS, 128), 1) // TOK == slot
    pieces = three_pieces(jnp.where(mine, logs4, 0.0)) + three_pieces(jnp.where(mine, deltas, 0.0))
    rows[...] = jnp.zeros_like(rows)
    for h in range(HEADS):
        for n, piece in enumerate(pieces):
            rows[h, n : n + 1, :] = piece[h : h + 1, :]
    for h in range(HEADS):
        out[h, 128:136, :] = rows[h].astype(BF16)


def unpack_body(got, qg, kv):
    for o in range(HEADS):
        qg[o * TOK : (o + 1) * TOK, :] = got[o, 0:32, :]
        qg[NEAR + o * TOK : NEAR + (o + 1) * TOK, :] = got[o, 32:64, :]
        kv[o * TOK : (o + 1) * TOK, :] = got[o, 64:96, :]
        kv[NEAR + o * TOK : NEAR + (o + 1) * TOK, :] = got[o, 96:128, :]
    for a in range(4):
        total = got[4 * a, 128:136, :].astype(F32)
        for j in range(1, 4):
            total = total + got[4 * a + j, 128:136, :].astype(F32)
        qg[2 * NEAR + 8 * a : 2 * NEAR + 8 * a + 8, :] = total.astype(BF16)


def one_block(q, g, logs, deltas, keys, values, dk_in, dv_in, dk, dv):
    total = None
    for base, size in ((0, NEAR), (NEAR, 2 * OWN - NEAR)):
        k, v = keys[base : base + size, :], values[base : base + size, :]
        weights = jnp.exp2(nt(k, q) * (SCALE * LOG2E) - logs)
        mixed = (weights * (nt(v, g) - deltas)).astype(BF16)
        rows = slice(base, base + size)
        value_part, key_part = nn(weights.astype(BF16), g), nn(mixed, q)
        dv[rows, :] = value_part if dv_in is None else dv_in[rows, :] + value_part
        dk[rows, :] = key_part if dk_in is None else dk_in[rows, :] + key_part
        part = tn(mixed, k)
        total = part if total is None else total + part
    return total * SCALE


def block_operands(qg):
    ld = qg[2 * NEAR : 2 * NEAR + 32, :].astype(F32)
    logs = jnp.concatenate(
        [ld[8 * a : 8 * a + 1] + ld[8 * a + 1 : 8 * a + 2] + ld[8 * a + 2 : 8 * a + 3] for a in range(4)],
        axis=1,
    )
    deltas = jnp.concatenate(
        [ld[8 * a + 3 : 8 * a + 4] + ld[8 * a + 4 : 8 * a + 5] + ld[8 * a + 5 : 8 * a + 6] for a in range(4)],
        axis=1,
    )
    return qg[0:NEAR, :], qg[NEAR : 2 * NEAR, :], logs, deltas


def text_body(kv_own, kv_other, text_k, text_v, text_q, text_g, text_ld, dq_text, dk, dv, keys, values, tq, tg):
    z, side = place()
    for target, start, text in ((keys, 0, text_k), (values, NEAR, text_v)):
        target[0:NEAR, :] = kv_own[start : start + NEAR, :]
        target[NEAR : 2 * NEAR, :] = kv_other[start : start + NEAR, :]
        target[2 * NEAR : 2 * OWN, :] = text[pl.ds(pl.multiple_of(z * 64, 64), 2 * TOK), :]
    for n in range(RING):
        rows = pl.ds(pl.multiple_of(n * 64 + side * TOK, TOK), TOK)
        tq[n * TOK : (n + 1) * TOK, :] = text_q[rows, :]
        tg[n * TOK : (n + 1) * TOK, :] = text_g[rows, :]
    logs, deltas = text_ld[pl.ds(side, 1), :], text_ld[pl.ds(2 + side, 1), :]
    dq_text[...] = one_block(tq[...], tg[...], logs, deltas, keys, values, None, None, dk, dv).astype(BF16)


def own_body(keys, values, qg, dk_in, dv_in, dq, dk, dv, send):
    _, side = place()
    q, g, logs, deltas = block_operands(qg)
    dq[...] = one_block(q, g, logs, deltas, keys, values, dk_in, dv_in, dk, dv)
    text = pl.ds(pl.multiple_of(2 * NEAR + (1 - side) * TOK, TOK), TOK)
    for source, lanes, factor in ((dk, slice(0, 128), SCALE), (dv, slice(128, 256), 1.0)):
        send[0:NEAR, lanes] = (source[NEAR : 2 * NEAR, :] * factor).astype(BF16)
        send[NEAR:OWN, lanes] = (source[text, :] * factor).astype(BF16)


def far_body(step, offset, *refs):
    keys, values, dq_text, qg, dk_in, dv_in = refs[:6]
    first, refs = (refs[6], refs[7:]) if step == 3 else (None, refs[6:])
    dq, dk, dv = refs[:3]
    z, _ = place()
    q, g, logs, deltas = block_operands(qg)
    dq[0:NEAR, :] = one_block(q, g, logs, deltas, keys, values, dk_in, dv_in, dk, dv).astype(dq.dtype)
    owner = lax.rem(z + offset, RING)
    text = dq_text[pl.ds(pl.multiple_of(owner * TOK, TOK), TOK), :]
    dq[NEAR:OWN, :] = text.astype(dq.dtype)
    if step == 3:
        dq[OWN : 2 * OWN, :] = first[...]


def mid_body(mine, *refs):
    total = mine[...]
    for got in refs[:-1]:
        total = total + got[0:OWN, :].astype(F32)
    refs[-1][...] = total.astype(BF16)


def join_body(dq, dq_text, dk, dv, kv_got, from_low, from_high, *refs):
    gots = refs[:2]
    out, out_q, out_k, out_v = refs[2:]
    z, side = place()

    def arrived(total, start, size):
        for got, base in ((from_low, OWN), (from_high, OWN), *((got, 0) for got in gots)):
            total = total + got[base + start : base + start + size, :].astype(F32)
        return total.astype(BF16)

    for o in range(HEADS):
        at = slice(o * TOK, (o + 1) * TOK)
        out[o, 0:32, :] = arrived(dq[at, :], o * TOK, TOK)
        out[o, 32:64, :] = (dk[at, :] * SCALE + kv_got[at, 0:128].astype(F32)).astype(BF16)
        out[o, 64:96, :] = (dv[at, :] + kv_got[at, 128:256].astype(F32)).astype(BF16)
    own_text = dq_text[pl.ds(pl.multiple_of(z * TOK, TOK), TOK), :].astype(F32)
    out_q[...] = arrived(own_text, NEAR, TOK)
    text = pl.ds(pl.multiple_of(2 * NEAR + side * TOK, TOK), TOK)
    out_k[...] = (dk[text, :] * SCALE + kv_got[NEAR:OWN, 0:128].astype(F32)).astype(BF16)
    out_v[...] = (dv[text, :] + kv_got[NEAR:OWN, 128:256].astype(F32)).astype(BF16)


def spread_body(got, dq, dk, dv):
    for h in range(HEADS):
        cols = slice(h * 128, (h + 1) * 128)
        dq[:, cols] = got[h, 0:32, :]
        dk[:, cols] = got[h, 32:64, :]
        dv[:, cols] = got[h, 64:96, :]


def kernel(body, outs, count, flops=0, scratch=(), aliases=None, limit=VMEM_LIMIT):
    return pl.pallas_call(
        body,
        out_shape=outs,
        in_specs=count if isinstance(count, list) else [VM] * count,
        out_specs=jax.tree.map(lambda _: VM, outs),
        scratch_shapes=scratch,
        input_output_aliases=aliases or {},
        cost_estimate=pl.CostEstimate(flops=flops, bytes_accessed=1 << 20, transcendentals=0),
        compiler_params=pltpu.CompilerParams(vmem_limit_bytes=limit),
    )


def sds(shape, dtype=BF16):
    return jax.ShapeDtypeStruct(shape, dtype)


def block_flops(queries):
    return 10 * queries * 2 * OWN * HEAD_DIM


def shards(
    query_image,
    key_image,
    value_image,
    attended_image,
    upstream_image,
    logsum_image,
    query_text,
    key_text,
    value_text,
    attended_text,
    upstream_text,
    logsum_text,
):
    def along_ring(x, step):
        pairs = [(2 * z + side, 2 * ((z + step) % RING) + side) for z in range(RING) for side in range(2)]
        return lax.ppermute(x, "inner", pairs)

    def exchanged(x):
        return lax.all_to_all(x, "outer", split_axis=0, concat_axis=0, tiled=True)

    def across(x):
        return lax.ppermute(x, "inner", [(n, n ^ 1) for n in range(2 * RING)])

    packed = kernel(
        pack_body,
        sds((HEADS, CHUNK, 128)),
        [HB] * 6,
        scratch=[pltpu.VMEM((HEADS, 8, 128), F32)]
        + [pltpu.VMEM((TOK, HEADS * 128), BF16)] * 5
        + [pltpu.VMEM((HEADS, TOK), F32), pltpu.SemaphoreType.DMA((6,))],
        limit=WHOLE_VMEM,
    )(query_image, key_image, value_image, attended_image, upstream_image, logsum_image.T)
    got = exchanged(packed)
    qg, kv = kernel(unpack_body, [sds((2 * NEAR + 32, 128)), sds((2 * NEAR, 128))], 1)(got)

    text_delta = jnp.sum(upstream_text.astype(F32) * attended_text.astype(F32), axis=1)
    text_ld = jnp.stack([logsum_text[:, 0] * LOG2E, text_delta]).reshape(2, RING, 2, TOK)
    text_ld = text_ld.transpose(0, 2, 1, 3).reshape(4, RING * TOK)

    kv_other = across(kv)
    acc = sds((2 * OWN, 128), F32)
    dq_text, dk, dv, keys, values = kernel(
        text_body,
        [sds((RING * TOK, 128)), acc, acc, sds((2 * OWN, 128)), sds((2 * OWN, 128))],
        7,
        flops=block_flops(RING * TOK),
        scratch=[pltpu.VMEM((RING * TOK, 128), BF16)] * 2,
    )(kv, kv_other, key_text, value_text, query_text, upstream_text, text_ld)

    up = down = qg
    parts = {}
    for step in range(1, 5):
        part = {1: sds((OWN, 128)), 2: sds((OWN, 128), F32), 3: sds((2 * OWN, 128)), 4: sds((OWN, 128))}[step]
        parts[step] = []
        up = along_ring(up, 1)
        if step < 4:
            down = along_ring(down, -1)
        for n, moved in enumerate((up, down) if step < 4 else (up,)):
            result = kernel(
                functools.partial(far_body, step, step if n else RING - step),
                [part, acc, acc],
                7 if step == 3 else 6,
                flops=block_flops(NEAR),
                aliases={4: 1, 5: 2},
            )(keys, values, dq_text, moved, dk, dv, *(parts[1][n : n + 1] if step == 3 else ()))
            parts[step].append(result[0])
            dk, dv = result[1:3]
    dq, dk, dv, send = kernel(
        own_body, [sds((NEAR, 128), F32), acc, acc, sds((OWN, 256))], 5, flops=block_flops(NEAR), aliases={3: 1, 4: 2}
    )(keys, values, qg, dk, dv)
    kv_got = across(send)
    from_high = along_ring(parts[3][0], -1)
    from_low = along_ring(parts[3][1], 1)
    from_far = along_ring(parts[4][0], -2)
    low, high = parts[2]
    high = kernel(mid_body, sds((OWN, 128)), 2)(high, from_low)
    back2 = along_ring(high, 2)
    low = kernel(mid_body, sds((OWN, 128)), 3)(low, from_high, from_far)
    back6 = along_ring(low, -2)

    joined, text_dq, text_dk, text_dv = kernel(
        join_body, [sds((HEADS, 96, 128)), sds((TOK, 128)), sds((TOK, 128)), sds((TOK, 128))], 9
    )(dq, dq_text, dk, dv, kv_got, from_low, from_high, back6, back2)
    home = exchanged(joined)
    image = kernel(spread_body, [sds((TOK, HEADS * 128))] * 3, 1)(home)
    return (*image, text_dq, text_dk, text_dv)


def solution(mesh):
    image = P(("outer", "inner"), None)
    text = P(None, "outer")
    share = P("inner", "outer")

    return jax.shard_map(
        shards,
        mesh=mesh,
        in_specs=(image,) * 6 + (text,) * 6,
        out_specs=(image,) * 3 + (share,) * 3,
        check_vma=False,
    )
```
